32 devices in a mesh: rep: 1, dp: 32 (over x, y, z, core).
Axes of the slice: x: 2, y: 2, z: 4, core: 2. Of those that a mesh axis runs over, the one named last changes fastest.
Arguments:
- g_w_gate: bfloat16 [32, 2, 1024, 3328], P(('rep', 'dp'))
- g_w_up: bfloat16 [32, 2, 1024, 3328], P(('rep', 'dp'))
- g_w_down: bfloat16 [32, 2, 3328, 1024], P(('rep', 'dp'))
- w_gate: bfloat16 [2, 1024, 3328], replicated
- w_up: bfloat16 [2, 1024, 3328], replicated
- w_down: bfloat16 [2, 3328, 1024], replicated
- m_w_gate: float32 [2, 1024, 3328], P(None, 'dp')
- m_w_up: float32 [2, 1024, 3328], P(None, 'dp')
- m_w_down: float32 [2, 3328, 1024], P(None, 'dp')
- v_w_gate: float32 [2, 1024, 3328], P(None, 'dp')
- v_w_up: float32 [2, 1024, 3328], P(None, 'dp')
- v_w_down: float32 [2, 3328, 1024], P(None, 'dp')
Outputs:
- output 1: bfloat16 [2, 1024, 3328], P('rep')
- output 2: bfloat16 [2, 1024, 3328], P('rep')
- output 3: bfloat16 [2, 3328, 1024], P('rep')
- output 4: float32 [2, 1024, 3328], P('rep', 'dp')
- output 5: float32 [2, 1024, 3328], P('rep', 'dp')
- output 6: float32 [2, 3328, 1024], P('rep', 'dp')
- output 7: float32 [2, 1024, 3328], P('rep', 'dp')
- output 8: float32 [2, 1024, 3328], P('rep', 'dp')
- output 9: float32 [2, 3328, 1024], P('rep', 'dp')
All inputs are finite; a program needn't handle non-finite values.
Results may differ from the reference program's by a relative error of at most 0.022.
Values are sent between devices in bfloat16 or wider.
A program may use at most 2 GiB of HBM per device.

```python
import jax
import jax.numpy as jnp
from jax import lax

DEVICES = 32
D = 1024
FF = 3328
LAYERS = 2
NAMES = ("w_gate", "w_up", "w_down")
SHAPES = {"w_gate": (LAYERS, D, FF), "w_up": (LAYERS, D, FF), "w_down": (LAYERS, FF, D)}


def setup_inputs(seed: int = 0, part: int = 0) -> dict:
    kz, *keys = jax.random.split(jax.random.key(seed), 1 + 5 * len(NAMES))
    loud = 2.0 ** jax.random.uniform(kz, (), jnp.float32, -1.0, 1.0)
    drawn = {}
    for name, key, both in zip(NAMES, keys[:3], keys[3:6], strict=True):
        own = jax.random.normal(jax.random.fold_in(key, part), (DEVICES, *SHAPES[name]), jnp.float32)
        shared = jax.random.normal(jax.random.fold_in(both, part), SHAPES[name], jnp.float32)
        drawn["g_" + name] = (loud * (0.7 * shared / DEVICES + 0.7 * own * DEVICES**-0.5)).astype(jnp.bfloat16)
    for name, key in zip(NAMES, keys[6:9], strict=True):
        drawn[name] = (jax.random.normal(key, SHAPES[name], jnp.float32) * SHAPES[name][1] ** -0.5).astype(jnp.bfloat16)
    for name, key in zip(NAMES, keys[9:12], strict=True):
        drawn["m_" + name] = loud * 0.5 * jax.random.normal(key, SHAPES[name], jnp.float32)
    for name, key in zip(NAMES, keys[12:15], strict=True):
        drawn["v_" + name] = loud * loud * jax.random.uniform(key, SHAPES[name], jnp.float32, 0.5, 1.5)
    return drawn


def adamw(w, m, v, g):
    m = 0.9 * m + 0.1 * g
    v = 0.95 * v + 0.05 * g * g
    step = m * lax.rsqrt(v + 1e-8) + 0.1 * w
    return (w - 0.02 * step).astype(jnp.bfloat16), m, v


def clipped(gradients, sum_of_squares, count):
    factor = jnp.minimum(1.0, 0.5 * lax.rsqrt(sum_of_squares / count + 1e-30))
    return [g * factor for g in gradients]


def reference(g_w_gate, g_w_up, g_w_down, w_gate, w_up, w_down, m_w_gate, m_w_up, m_w_down, v_w_gate, v_w_up, v_w_down):
    def total(terms):
        return lax.scan(lambda so_far, term: (so_far + term.astype(jnp.float32), None), jnp.zeros(terms.shape[1:], jnp.float32), terms)[0]

    gradients = [total(terms).astype(jnp.bfloat16).astype(jnp.float32) for terms in (g_w_gate, g_w_up, g_w_down)]
    gradients = clipped(gradients, sum(jnp.sum(g * g) for g in gradients), sum(g.size for g in gradients))
    new = [
        adamw(w.astype(jnp.float32), m, v, g)
        for w, m, v, g in zip((w_gate, w_up, w_down), (m_w_gate, m_w_up, m_w_down), (v_w_gate, v_w_up, v_w_down), gradients, strict=True)
    ]
    return tuple(one[which] for which in range(3) for one in new)
```

```python
import functools

import jax
import jax.numpy as jnp
from jax import lax
from jax.experimental import pallas as pl
from jax.experimental.pallas import tpu as pltpu
from jax.sharding import PartitionSpec as P

MESH = pl.DeviceIdType.MESH
CHIPS = 16
TILES, PART = 52, 13
ROUNDS = 12
START, COUNT = (0, 8, 12, 14), (8, 4, 2, 1)
SUM_LAG = (0, 1, 2, 3, 4)
GATHER_LAG = (0, 1, 2, 3, 4)


def view(t):
    layers, rows, columns = t.shape
    return t.reshape(layers, rows // 8, 8, columns // 128, 128).transpose(0, 1, 3, 2, 4).reshape(layers, -1, TILES, 16, 128)


def unview(t, shape):
    layers, rows, columns = shape
    return t.reshape(layers, rows // 8, columns // 128, 8, 128).transpose(0, 1, 3, 2, 4).reshape(shape)


def place():
    me = lax.axis_index("dp")
    return me, me // 2, me % 2


def is_down(t):
    return (t % 3) // 2


def source(t):
    i = 2 * (t // 3) + t % 3
    return i // 4, i % 4, t // 3


def bits(t, a):
    d = is_down(t)
    first, last = (8, 4) if a == 0 else (4, 8)
    return first, 1 + (last - 1) * d, 2 - d, last - (last - 2) * d


def bit(k, b):
    return (k // b) % 2


def flip(k, b):
    return k + (1 - 2 * bit(k, b)) * b


def copy_to(src, dst, send, recv, chip, core):
    return pltpu.make_async_remote_copy(src_ref=src, dst_ref=dst, send_sem=send, recv_sem=recv, device_id={"dp": 2 * chip + core}, device_id_type=MESH)


def sum_kernel(gate, up, down, out, norm, own, pair, slots, squares, parts, own_sem, pair_send, pair_recv, send, recv, norm_send, norm_recv):
    me, k, c = place()

    def arrays(t, a, core):
        if t % 3 == 2:
            return down.at[a, :, core, pl.ds(source(t)[2] * PART, PART)]
        layer, part, _ = source(t)
        return (gate, up)[a].at[layer, :, core, pl.ds(part * PART, PART)]

    for t in range(ROUNDS):
        for a in range(2):
            copy_to(arrays(t, a, 1 - c), pair.at[t, a], pair_send.at[t, a], pair_recv.at[t, a], k, 1 - c).start()
            pltpu.make_async_copy(arrays(t, a, c), own.at[t, a], own_sem.at[t, a]).start()
    squares[...] = jnp.zeros_like(squares)

    def await_slots(t, a, s):
        got = slots.at[t, a, pl.ds(START[s], COUNT[s])]
        pltpu.make_async_copy(got, got, recv.at[t, a, s]).wait()

    def total(t, a, s, chip):
        b = bits(t, a)
        so_far = own[t, a, chip].astype(jnp.float32) + pair[t, a, chip].astype(jnp.float32)
        for i in range(s):
            index = START[i]
            for j in range(i + 1, 4):
                index = index + bit(chip, b[j]) * 2 ** (3 - j)
            so_far = so_far + slots[t, a, index].astype(jnp.float32)
        return so_far

    def stage(t, a, s):
        b = bits(t, a)
        other = flip(k, b[s])
        if s == 0:
            pltpu.make_async_copy(own.at[t, a], own.at[t, a], own_sem.at[t, a]).wait()
            pltpu.make_async_copy(pair.at[t, a], pair.at[t, a], pair_recv.at[t, a]).wait()
        else:
            await_slots(t, a, s - 1)
        base = other
        for i in range(s + 1, 4):
            base = base - bit(other, b[i]) * b[i]

        def chip_of(j):
            chip = base
            for i in range(s + 1, 4):
                chip = chip + bit(j, 2 ** (3 - i)) * b[i]
            return chip

        def add(j, _):
            chip = chip_of(j)
            own[t, a, chip] = total(t, a, s, chip).astype(jnp.bfloat16)
            return 0

        def go(j, _):
            copy_to(own.at[t, a, chip_of(j)], slots.at[t, a, START[s] + j], send.at[t, a, s], recv.at[t, a, s], other, c).start()
            return 0

        lax.fori_loop(0, COUNT[s], add, 0)
        lax.fori_loop(0, COUNT[s], go, 0)

    def finish(t, a):
        await_slots(t, a, 3)
        g = total(t, a, 4, k).astype(jnp.bfloat16)
        out[t, a] = g
        g = g.astype(jnp.float32)
        squares[...] += jnp.sum(g * g, axis=0)

    def step(now, _):
        for s in range(5):
            t = now - SUM_LAG[s]

            @pl.when((t >= 0) & (t < ROUNDS))
            def _():
                for a in range(2):
                    if s < 4:
                        stage(t, a, s)
                    else:
                        finish(t, a)

        return 0

    lax.fori_loop(0, ROUNDS + SUM_LAG[4], step, 0)

    mine = parts.at[me]
    mine[...] = squares[...]

    def tell(i, _):
        to = (me + i) % 32
        pltpu.make_async_remote_copy(src_ref=squares, dst_ref=mine, send_sem=norm_send, recv_sem=norm_recv, device_id={"dp": to}, device_id_type=MESH).start()
        return 0

    lax.fori_loop(1, 32, tell, 0)
    others = parts.at[pl.ds(0, 31)]
    pltpu.make_async_copy(others, others, norm_recv).wait()
    norm[...] = jnp.sum(parts[...], axis=0)
    pltpu.make_async_copy(others, others, norm_send).wait()

    def drain(t, _):
        for a in range(2):
            pltpu.make_async_copy(pair.at[t, a], pair.at[t, a], pair_send.at[t, a]).wait()
            for s in range(4):
                sent = slots.at[t, a, pl.ds(START[s], COUNT[s])]
                pltpu.make_async_copy(sent, sent, send.at[t, a, s]).wait()
        return 0

    lax.fori_loop(0, ROUNDS, drain, 0)


def gather_kernel(new, gate, up, down, own_sem, pair_send, pair_recv, send, recv):
    _, k, c = place()

    def block(t, a, chip, core, count=None):
        chip = chip if count is None else pl.ds(chip, count)
        if t % 3 == 2:
            return down.at[a, chip, core, pl.ds(source(t)[2] * PART, PART)]
        layer, part, _ = source(t)
        return (gate, up)[a].at[layer, chip, core, pl.ds(part * PART, PART)]

    for t in range(ROUNDS):
        for a in range(2):
            pltpu.make_async_copy(new.at[t, a], block(t, a, k, c), own_sem.at[t, a]).start()

    def chips(t, a, s, at):
        b = bits(t, a)[::-1]
        base = at
        for i in range(s):
            base = base - bit(at, b[i]) * b[i]

        def chip_of(j):
            chip = base
            for i in range(s):
                chip = chip + bit(j, 2**i) * b[i]
            return chip

        return chip_of

    def whole(t, a, count):
        return block(t, a, 0, 0, count)

    def pass_on(t, a, s):
        if s == 0:
            of, count = chips(t, a, 0, k), 1
        else:
            of, count = chips(t, a, s - 1, flip(k, bits(t, a)[4 - s])), 2 ** (s - 1)

        def go(j, _):
            one = block(t, a, of(j), c)
            copy_to(one, one, pair_send.at[t, a], pair_recv.at[t, a], k, 1 - c).start()
            return 0

        lax.fori_loop(0, count, go, 0)

    def stage(t, a, s):
        if s == 0:
            pltpu.make_async_copy(new.at[t, a], new.at[t, a], own_sem.at[t, a]).wait()
        else:
            got = whole(t, a, 2 ** (s - 1))
            pltpu.make_async_copy(got, got, recv.at[t, a, s - 1]).wait()
        if s < 4:
            of, other = chips(t, a, s, k), flip(k, bits(t, a)[3 - s])

            def go(j, _):
                one = block(t, a, of(j), c)
                copy_to(one, one, send.at[t, a, s], recv.at[t, a, s], other, c).start()
                return 0

            lax.fori_loop(0, 2**s, go, 0)
        pass_on(t, a, s)

    for now in range(ROUNDS + GATHER_LAG[4]):
        for s in range(5):
            t = now - GATHER_LAG[s]
            if 0 <= t < ROUNDS:
                for a in range(2):
                    stage(t, a, s)

    for t in range(ROUNDS):
        for a in range(2):
            pltpu.make_async_copy(whole(t, a, 16), whole(t, a, 16), pair_recv.at[t, a]).wait()
            pltpu.make_async_copy(whole(t, a, 16), whole(t, a, 16), pair_send.at[t, a]).wait()
            for s in range(4):
                pltpu.make_async_copy(whole(t, a, 2**s), whole(t, a, 2**s), send.at[t, a, s]).wait()


def adamw(w, m, v, g):
    m = 0.9 * m + 0.1 * g
    v = 0.95 * v + 0.05 * g * g
    step = m * lax.rsqrt(v + 1e-8) + 0.1 * w
    return (w - 0.02 * step).astype(jnp.bfloat16), m, v


def split(rounds):
    rounds = rounds.reshape(4, 3, 2, PART, 16, 128)
    sides = rounds[:, :2].reshape(2, 4, 2, PART, 16, 128)
    gate, up = (sides[:, :, a].reshape(2, TILES, 16, 128) for a in range(2))
    return gate, up, jnp.swapaxes(rounds[:, 2], 0, 1).reshape(2, TILES, 16, 128)


def merge(gate, up, down):
    sides = jnp.stack([one.reshape(8, PART, 16, 128) for one in (gate, up)], 1).reshape(4, 2, 2, PART, 16, 128)
    down = jnp.swapaxes(down.reshape(2, 4, PART, 16, 128), 0, 1)
    return jnp.concatenate([sides, down[:, None]], 1).reshape(ROUNDS, 2, PART, 16, 128)


def solution(mesh):
    hbm, vmem = pl.BlockSpec(memory_space=pl.ANY), pl.BlockSpec(memory_space=pltpu.VMEM)
    dma = pltpu.SemaphoreType.DMA
    params = pltpu.CompilerParams(has_side_effects=True, vmem_limit_bytes=67043328)

    def step(*arrays):
        terms, weights, m, v = (arrays[i : i + 3] for i in (0, 3, 6, 9))
        tile = (16, 128)
        terms = [view(t[0]).reshape(2, CHIPS, 2, TILES, *tile) for t in terms]
        summed, norm = pl.pallas_call(
            sum_kernel,
            out_shape=[jax.ShapeDtypeStruct((ROUNDS, 2, PART, *tile), jnp.bfloat16), jax.ShapeDtypeStruct(tile, jnp.float32)],
            in_specs=[hbm] * 3,
            out_specs=[vmem] * 2,
            scratch_shapes=[
                pltpu.VMEM((ROUNDS, 2, CHIPS, PART, *tile), jnp.bfloat16),
                pltpu.VMEM((ROUNDS, 2, CHIPS, PART, *tile), jnp.bfloat16),
                pltpu.VMEM((ROUNDS, 2, 15, PART, *tile), jnp.bfloat16),
                pltpu.VMEM(tile, jnp.float32),
                pltpu.VMEM((32, *tile), jnp.float32),
                dma((ROUNDS, 2)),
                dma((ROUNDS, 2)),
                dma((ROUNDS, 2)),
                dma((ROUNDS, 2, 4)),
                dma((ROUNDS, 2, 4)),
                dma,
                dma,
            ],
            compiler_params=params,
        )(*terms)
        count = 32 * sum(one.size for one in m)
        factor = jnp.minimum(1.0, 0.5 * lax.rsqrt(jnp.sum(norm) / count + 1e-30))
        me = lax.axis_index("dp")
        own = [lax.dynamic_index_in_dim(view(w), me, 1, False).astype(jnp.float32) for w in weights]
        g = [one.astype(jnp.float32) * factor for one in split(summed)]
        new = [adamw(w, view(m)[:, 0], view(v)[:, 0], g) for w, m, v, g in zip(own, m, v, g, strict=True)]
        whole = pl.pallas_call(
            gather_kernel,
            out_shape=[jax.ShapeDtypeStruct((2, CHIPS, 2, TILES, *tile), jnp.bfloat16)] * 3,
            in_specs=[vmem],
            out_specs=[hbm] * 3,
            scratch_shapes=[
                dma((ROUNDS, 2)),
                dma((ROUNDS, 2)),
                dma((ROUNDS, 2)),
                dma((ROUNDS, 2, 4)),
                dma((ROUNDS, 2, 4)),
            ],
            compiler_params=params,
        )(merge(*(one[0] for one in new)))
        whole = [unview(one, w.shape) for one, w in zip(whole, weights, strict=True)]
        return (*whole, *(unview(n[1], one.shape) for n, one in zip(new, m, strict=True)), *(unview(n[2], one.shape) for n, one in zip(new, v, strict=True)))

    all_of, cut = P(None, None, None), P(None, "dp", None)
    return jax.shard_map(
        step,
        mesh=mesh,
        in_specs=(P(("rep", "dp"), None, None, None),) * 3 + (all_of,) * 3 + (cut,) * 6,
        out_specs=(P("rep", None, None),) * 3 + (P("rep", "dp", None),) * 6,
        check_vma=False,
    )
```

```python
import functools

import jax
import jax.numpy as jnp
from jax import lax
from jax.experimental import pallas as pl
from jax.experimental.pallas import tpu as pltpu
from jax.sharding import PartitionSpec as P

MESH = pl.DeviceIdType.MESH
CHIPS = 16
ROWS, TILES, PART = 8, 104, 13
PARTS = TILES // PART
ROUNDS = 3 * PARTS
START, COUNT = (0, 8, 12, 14), (8, 4, 2, 1)
AHEAD = 3
SUM_LAG = (0, 1, 2, 3, 4)
GATHER_LAG = (0, 1, 2, 3, 4)


def view(t):
    layers, rows, columns = t.shape
    return t.reshape(layers, rows // 8, 8, columns // 128, 128).transpose(0, 1, 3, 2, 4).reshape(layers, -1, TILES, ROWS, 128)


def unview(t, shape):
    layers, rows, columns = shape
    return t.reshape(layers, rows // 8, columns // 128, 8, 128).transpose(0, 1, 3, 2, 4).reshape(shape)


def place():
    me = lax.axis_index("dp")
    return me, me // 2, me % 2


def is_down(t):
    return (t % 3) // 2


def source(t):
    i = 2 * (t // 3) + t % 3
    return i // PARTS, i % PARTS, t // 3


def bits(a):
    return ((8, 1, 4, 2), (4, 1, 8, 2))[a]


def by_kind(t, do):
    for down in (False, True):
        pl.when(is_down(t) == int(down))(functools.partial(do, down))


def bit(k, b):
    return (k // b) % 2


def flip(k, b):
    return k + (1 - 2 * bit(k, b)) * b


def copy_to(src, dst, send, recv, chip, core):
    return pltpu.make_async_remote_copy(src_ref=src, dst_ref=dst, send_sem=send, recv_sem=recv, device_id={"dp": 2 * chip + core}, device_id_type=MESH)


def sum_kernel(gate, up, down, gate_out, up_out, down_out, norm, own, pair, slots, squares, parts, own_sem, pair_send, pair_recv, send, recv, norm_send, norm_recv):
    me, k, c = place()

    def load(t):
        def go(w_down):
            layer, part, down_part = source(t)
            for a in range(2):
                ref, layer_a, part_a = (down, a, down_part) if w_down else ((gate, up)[a], layer, part)
                at = pl.ds(part_a * PART, PART)
                copy_to(ref.at[layer_a, :, 1 - c, at], pair.at[t, a], pair_send.at[t, a], pair_recv.at[t, a], k, 1 - c).start()
                pltpu.make_async_copy(ref.at[layer_a, :, c, at], own.at[t, a], own_sem.at[t, a]).start()

        by_kind(t, go)

    lax.fori_loop(0, AHEAD, lambda t, _: load(t), None)
    squares[...] = jnp.zeros_like(squares)

    def await_slots(t, a, s):
        got = slots.at[t, a, pl.ds(START[s], COUNT[s])]
        pltpu.make_async_copy(got, got, recv.at[t, a, s]).wait()

    def total(t, a, s, chip):
        b = bits(a)
        so_far = own[t, a, chip].astype(jnp.float32) + pair[t, a, chip].astype(jnp.float32)
        for i in range(s):
            index = START[i]
            for j in range(i + 1, 4):
                index = index + bit(chip, b[j]) * 2 ** (3 - j)
            so_far = so_far + slots[t, a, index].astype(jnp.float32)
        return so_far

    def stage(t, a, s):
        b = bits(a)
        other = flip(k, b[s])
        if s == 0:
            pltpu.make_async_copy(own.at[t, a], own.at[t, a], own_sem.at[t, a]).wait()
            pltpu.make_async_copy(pair.at[t, a], pair.at[t, a], pair_recv.at[t, a]).wait()
        else:
            await_slots(t, a, s - 1)
        base = other
        for i in range(s + 1, 4):
            base = base - bit(other, b[i]) * b[i]

        def chip_of(j):
            chip = base
            for i in range(s + 1, 4):
                chip = chip + bit(j, 2 ** (3 - i)) * b[i]
            return chip

        def add(j, _):
            chip = chip_of(j)
            own[t, a, chip] = total(t, a, s, chip).astype(jnp.bfloat16)
            return 0

        def go(j, _):
            copy_to(own.at[t, a, chip_of(j)], slots.at[t, a, START[s] + j], send.at[t, a, s], recv.at[t, a, s], other, c).start()
            return 0

        lax.fori_loop(0, COUNT[s], add, 0)
        lax.fori_loop(0, COUNT[s], go, 0)

    def finish(t, a):
        await_slots(t, a, 3)
        g = total(t, a, 4, k).astype(jnp.bfloat16)

        def put(w_down):
            layer, part, down_part = source(t)
            out, layer, part = (down_out, a, down_part) if w_down else ((gate_out, up_out)[a], layer, part)
            out[layer, pl.ds(part * PART, PART)] = g

        by_kind(t, put)
        g = g.astype(jnp.float32)
        squares[...] += jnp.sum(g * g, axis=0)

    def step(now, _):
        pl.when(now + AHEAD < ROUNDS)(lambda: load(now + AHEAD))
        for s in range(5):
            t = now - SUM_LAG[s]

            @pl.when((t >= 0) & (t < ROUNDS))
            def _():
                for a in range(2):
                    if s < 4:
                        stage(t, a, s)
                    else:
                        finish(t, a)

        return 0

    lax.fori_loop(0, ROUNDS + SUM_LAG[4], step, 0)

    mine = parts.at[me]
    mine[...] = squares[...]

    def tell(i, _):
        to = (me + i) % 32
        pltpu.make_async_remote_copy(src_ref=squares, dst_ref=mine, send_sem=norm_send, recv_sem=norm_recv, device_id={"dp": to}, device_id_type=MESH).start()
        return 0

    lax.fori_loop(1, 32, tell, 0)
    others = parts.at[pl.ds(0, 31)]
    pltpu.make_async_copy(others, others, norm_recv).wait()
    norm[...] = jnp.sum(parts[...], axis=0)
    pltpu.make_async_copy(others, others, norm_send).wait()

    def drain(t, _):
        for a in range(2):
            pltpu.make_async_copy(pair.at[t, a], pair.at[t, a], pair_send.at[t, a]).wait()
            for s in range(4):
                sent = slots.at[t, a, pl.ds(START[s], COUNT[s])]
                pltpu.make_async_copy(sent, sent, send.at[t, a, s]).wait()
        return 0

    lax.fori_loop(0, ROUNDS, drain, 0)


def gather_kernel(gate_new, up_new, down_new, gate, up, down, own_sem, pair_send, pair_recv, send, recv):
    _, k, c = place()

    def block(w_down, t, a, chip, core, count=None):
        chip = chip if count is None else pl.ds(chip, count)
        layer, part, down_part = source(t)
        ref, layer, part = (down, a, down_part) if w_down else ((gate, up)[a], layer, part)
        return ref.at[layer, chip, core, pl.ds(part * PART, PART)]

    def chips(a, s, at):
        b = bits(a)[::-1]
        base = at
        for i in range(s):
            base = base - bit(at, b[i]) * b[i]

        def chip_of(j):
            chip = base
            for i in range(s):
                chip = chip + bit(j, 2**i) * b[i]
            return chip

        return chip_of

    def own_block(w_down, t, a):
        layer, part, down_part = source(t)
        ref, layer, part = (down_new, a, down_part) if w_down else ((gate_new, up_new)[a], layer, part)
        return pltpu.make_async_copy(ref.at[layer, pl.ds(part * PART, PART)], block(w_down, t, a, k, c), own_sem.at[t, a])

    def start_own(t, _):
        by_kind(t, lambda w_down: [own_block(w_down, t, a).start() for a in range(2)] and None)
        return 0

    lax.fori_loop(0, ROUNDS, start_own, 0)

    def stage(w_down, t, a, s):
        if s == 0:
            own_block(w_down, t, a).wait()
            fresh, count = chips(a, 0, k), 1
        else:
            count = 2 ** (s - 1)
            got = block(w_down, t, a, 0, 0, count)
            pltpu.make_async_copy(got, got, recv.at[t, a, s - 1]).wait()
            fresh = chips(a, s - 1, flip(k, bits(a)[4 - s]))
        if s < 4:
            of, other = chips(a, s, k), flip(k, bits(a)[3 - s])

            def go(j, _):
                one = block(w_down, t, a, of(j), c)
                copy_to(one, one, send.at[t, a, s], recv.at[t, a, s], other, c).start()
                return 0

            lax.fori_loop(0, 2**s, go, 0)

        def share(j, _):
            one = block(w_down, t, a, fresh(j), c)
            copy_to(one, one, pair_send.at[t, a], pair_recv.at[t, a], k, 1 - c).start()
            return 0

        lax.fori_loop(0, count, share, 0)

    def step(now, _):
        for s in range(5):
            t = now - GATHER_LAG[s]

            @pl.when((t >= 0) & (t < ROUNDS))
            def _():
                def go(w_down):
                    for a in range(2):
                        stage(w_down, t, a, s)

                by_kind(t, go)

        return 0

    lax.fori_loop(0, ROUNDS + GATHER_LAG[4], step, 0)

    def drain(t, _):
        for a in range(2):
            for sems, s in ((pair_recv.at[t, a], 4), (pair_send.at[t, a], 4), *((send.at[t, a, s], s) for s in range(4))):
                size = gate.at[0, pl.ds(0, 2**s), 0, pl.ds(0, PART)]
                pltpu.make_async_copy(size, size, sems).wait()
        return 0

    lax.fori_loop(0, ROUNDS, drain, 0)


def update_kernel(count, g, norm, w, m, v, w_new, m_new, v_new, w_now, m_now, v_now, got, put):
    me, _, _ = place()
    units = [(i, layer) for i in range(3) for layer in range(2)]

    def moves(u, inward):
        i, layer = units[u]
        come = ((w[i].at[layer, me], w_now), (m[i].at[layer], m_now), (v[i].at[layer], v_now))
        leave = (w_new[i].at[layer], m_new[i].at[layer], v_new[i].at[layer])
        if inward:
            return [pltpu.make_async_copy(there, here.at[u], got.at[u, n]) for n, (there, here) in enumerate(come)]
        return [pltpu.make_async_copy(here.at[u], there, put.at[u, n]) for n, ((_, here), there) in enumerate(zip(come, leave, strict=True))]

    for u in range(6):
        for one in moves(u, True):
            one.start()
    squares = jnp.full((ROWS, 128), jnp.sum(norm[...]), jnp.float32)
    factor = jnp.minimum(1.0, 0.5 * lax.rsqrt(squares / count + 1e-30))
    for u, (i, layer) in enumerate(units):
        for one in moves(u, True):
            one.wait()

        def go(j, _):
            at = pl.ds(j * PART, PART)
            gradient = g[i][layer, at].astype(jnp.float32) * factor
            w_now[u, at], m_now[u, at], v_now[u, at] = adamw(w_now[u, at].astype(jnp.float32), m_now[u, at], v_now[u, at], gradient)
            return 0

        lax.fori_loop(0, PARTS, go, 0)
        for one in moves(u, False):
            one.start()
    for u in range(6):
        for one in moves(u, False):
            one.wait()


def store_kernel(*refs):
    copies = [pltpu.make_async_copy(refs[i].at[layer], refs[3 + i].at[layer], refs[6].at[i, layer]) for i in range(3) for layer in range(2)]
    for one in copies:
        one.start()
    for one in copies:
        one.wait()


def adamw(w, m, v, g):
    m = 0.9 * m + 0.1 * g
    v = 0.95 * v + 0.05 * g * g
    step = m * lax.rsqrt(v + 1e-8) + 0.1 * w
    return (w - 0.02 * step).astype(jnp.bfloat16), m, v


def solution(mesh):
    hbm, vmem, fixed = (pl.BlockSpec(memory_space=one) for one in (pl.ANY, pltpu.VMEM, pltpu.HBM))
    dma = pltpu.SemaphoreType.DMA
    small = pltpu.CompilerParams(vmem_limit_bytes=1 << 20)
    params = pltpu.CompilerParams(has_side_effects=True, vmem_limit_bytes=67043328)

    def step(*arrays):
        terms, weights, m, v = (arrays[i : i + 3] for i in (0, 3, 6, 9))
        tile = (ROWS, 128)
        terms = [view(t[0]).reshape(2, CHIPS, 2, TILES, *tile) for t in terms]
        *g, norm = pl.pallas_call(
            sum_kernel,
            out_shape=[*[jax.ShapeDtypeStruct((2, TILES, *tile), jnp.bfloat16)] * 3, jax.ShapeDtypeStruct(tile, jnp.float32)],
            in_specs=[hbm] * 3,
            out_specs=[vmem] * 4,
            scratch_shapes=[
                pltpu.VMEM((ROUNDS, 2, CHIPS, PART, *tile), jnp.bfloat16),
                pltpu.VMEM((ROUNDS, 2, CHIPS, PART, *tile), jnp.bfloat16),
                pltpu.VMEM((ROUNDS, 2, 15, PART, *tile), jnp.bfloat16),
                pltpu.VMEM(tile, jnp.float32),
                pltpu.VMEM((32, *tile), jnp.float32),
                dma((ROUNDS, 2)),
                dma((ROUNDS, 2)),
                dma((ROUNDS, 2)),
                dma((ROUNDS, 2, 4)),
                dma((ROUNDS, 2, 4)),
                dma,
                dma,
            ],
            compiler_params=params,
        )(*terms)
        count = 32 * sum(one.size for one in m)

        def update(*refs):
            threes = [refs[i : i + 3] for i in (0, 4, 7, 10, 13, 16, 19)]
            update_kernel(count, threes[0], refs[3], *threes[1:], *refs[22:])

        mine = (2, TILES, *tile)
        *new, m0, m1, m2, v0, v1, v2 = pl.pallas_call(
            update,
            out_shape=[jax.ShapeDtypeStruct(mine, jnp.bfloat16)] * 3 + [jax.ShapeDtypeStruct(mine, jnp.float32)] * 6,
            in_specs=[vmem] * 4 + [fixed] * 9,
            out_specs=[fixed] * 9,
            scratch_shapes=[
                pltpu.VMEM((6, TILES, *tile), jnp.bfloat16),
                pltpu.VMEM((6, TILES, *tile), jnp.float32),
                pltpu.VMEM((6, TILES, *tile), jnp.float32),
                dma((6, 3)),
                dma((6, 3)),
            ],
        )(*g, norm, *(view(one) for one in weights), *(view(one)[:, 0] for one in (*m, *v)))
        whole = pl.pallas_call(
            gather_kernel,
            out_shape=[jax.ShapeDtypeStruct((2, CHIPS, 2, TILES, *tile), jnp.bfloat16)] * 3,
            in_specs=[vmem] * 3,
            out_specs=[hbm] * 3,
            scratch_shapes=[
                dma((ROUNDS, 2)),
                dma((ROUNDS, 2)),
                dma((ROUNDS, 2)),
                dma((ROUNDS, 2, 4)),
                dma((ROUNDS, 2, 4)),
            ],
            compiler_params=pltpu.CompilerParams(has_side_effects=True, vmem_limit_bytes=4 << 20),
        )(*new)
        whole = pl.pallas_call(store_kernel, out_shape=[jax.ShapeDtypeStruct(one.shape, one.dtype) for one in whole], in_specs=[hbm] * 3, out_specs=[hbm] * 3, scratch_shapes=[dma((3, 2))], compiler_params=small)(*whole)
        whole = [unview(one, w.shape) for one, w in zip(whole, weights, strict=True)]
        moments = [unview(one, like.shape) for one, like in zip((m0, m1, m2, v0, v1, v2), (*m, *v), strict=True)]
        return (*whole, *moments)

    all_of, cut = P(None, None, None), P(None, "dp", None)
    return jax.shard_map(
        step,
        mesh=mesh,
        in_specs=(P(("rep", "dp"), None, None, None),) * 3 + (all_of,) * 3 + (cut,) * 6,
        out_specs=(P("rep", None, None),) * 3 + (P("rep", "dp", None),) * 6,
        check_vma=False,
    )
```

```python
import functools

import jax
import jax.numpy as jnp
from jax import lax
from jax.experimental import pallas as pl
from jax.experimental.pallas import tpu as pltpu
from jax.sharding import PartitionSpec as P

MESH = pl.DeviceIdType.MESH
CHIPS = 16
ROWS, TILES, PART = 8, 104, 13
PARTS = TILES // PART
ROUNDS = 3 * PARTS
START, COUNT = (0, 8, 12, 14), (8, 4, 2, 1)
AHEAD = 3
LIMIT = 12
SUM_LAG = (0, 1, 2, 3, 4)
GATHER_LAG = (0, 1, 2, 3, 4)


def view(t):
    layers, rows, columns = t.shape
    return t.reshape(layers, rows // 8, 8, columns // 128, 128).transpose(0, 1, 3, 2, 4).reshape(layers, -1, TILES, ROWS, 128)


def unview(t, shape):
    layers, rows, columns = shape
    return t.reshape(layers, rows // 8, columns // 128, 8, 128).transpose(0, 1, 3, 2, 4).reshape(shape)


def place():
    me = lax.axis_index("dp")
    return me, me // 2, me % 2


def is_down(t):
    return (t % 3) // 2


def source(t):
    i = 2 * (t // 3) + t % 3
    return i // PARTS, i % PARTS, t // 3


def bits(a):
    return ((8, 1, 4, 2), (4, 1, 8, 2))[a]


def by_kind(t, do):
    for down in (False, True):
        pl.when(is_down(t) == int(down))(functools.partial(do, down))


def bit(k, b):
    return (k // b) % 2


def flip(k, b):
    return k + (1 - 2 * bit(k, b)) * b


def copy_to(src, dst, send, recv, chip, core):
    return pltpu.make_async_remote_copy(src_ref=src, dst_ref=dst, send_sem=send, recv_sem=recv, device_id={"dp": 2 * chip + core}, device_id_type=MESH)


def sum_kernel(gate, up, down, gate_out, up_out, down_out, norm, own, pair, slots, squares, parts, own_sem, pair_send, pair_recv, send, recv, norm_send, norm_recv):
    me, k, c = place()

    def load(t):
        def go(w_down):
            layer, part, down_part = source(t)
            for a in range(2):
                ref, layer_a, part_a = (down, a, down_part) if w_down else ((gate, up)[a], layer, part)
                at = pl.ds(part_a * PART, PART)
                copy_to(ref.at[layer_a, :, 1 - c, at], pair.at[t, a], pair_send.at[t, a], pair_recv.at[t, a], k, 1 - c).start()
                pltpu.make_async_copy(ref.at[layer_a, :, c, at], own.at[t, a], own_sem.at[t, a]).start()

        by_kind(t, go)

    lax.fori_loop(0, AHEAD, lambda t, _: load(t), None)
    squares[...] = jnp.zeros_like(squares)

    def await_slots(t, a, s):
        got = slots.at[t, a, pl.ds(START[s], COUNT[s])]
        pltpu.make_async_copy(got, got, recv.at[t, a, s]).wait()

    def total(t, a, s, chip):
        b = bits(a)
        so_far = own[t, a, chip].astype(jnp.float32) + pair[t, a, chip].astype(jnp.float32)
        for i in range(s):
            index = START[i]
            for j in range(i + 1, 4):
                index = index + bit(chip, b[j]) * 2 ** (3 - j)
            so_far = so_far + slots[t, a, index].astype(jnp.float32)
        return so_far

    def stage(t, a, s):
        b = bits(a)
        other = flip(k, b[s])
        if s == 0:
            pltpu.make_async_copy(own.at[t, a], own.at[t, a], own_sem.at[t, a]).wait()
            pltpu.make_async_copy(pair.at[t, a], pair.at[t, a], pair_recv.at[t, a]).wait()
        else:
            await_slots(t, a, s - 1)
        base = other
        for i in range(s + 1, 4):
            base = base - bit(other, b[i]) * b[i]

        def chip_of(j):
            chip = base
            for i in range(s + 1, 4):
                chip = chip + bit(j, 2 ** (3 - i)) * b[i]
            return chip

        def add(j, _):
            chip = chip_of(j)
            own[t, a, chip] = total(t, a, s, chip).astype(jnp.bfloat16)
            return 0

        def go(j, _):
            copy_to(own.at[t, a, chip_of(j)], slots.at[t, a, START[s] + j], send.at[t, a, s], recv.at[t, a, s], other, c).start()
            return 0

        lax.fori_loop(0, COUNT[s], add, 0)
        lax.fori_loop(0, COUNT[s], go, 0)

    def finish(t, a):
        await_slots(t, a, 3)
        g = total(t, a, 4, k).astype(jnp.bfloat16)

        def put(w_down):
            layer, part, down_part = source(t)
            out, layer, part = (down_out, a, down_part) if w_down else ((gate_out, up_out)[a], layer, part)
            out[layer, pl.ds(part * PART, PART)] = g

        by_kind(t, put)
        g = g.astype(jnp.float32)
        squares[...] += jnp.sum(g * g, axis=0)

    def step(now, _):
        pl.when(now + AHEAD < ROUNDS)(lambda: load(now + AHEAD))
        for s in range(5):
            t = now - SUM_LAG[s]

            @pl.when((t >= 0) & (t < ROUNDS))
            def _():
                for a in range(2):
                    if s < 4:
                        stage(t, a, s)
                    else:
                        finish(t, a)

        return 0

    lax.fori_loop(0, ROUNDS + SUM_LAG[4], step, 0)

    mine = parts.at[me]
    mine[...] = squares[...]

    def tell(i, _):
        to = (me + i) % 32
        pltpu.make_async_remote_copy(src_ref=squares, dst_ref=mine, send_sem=norm_send, recv_sem=norm_recv, device_id={"dp": to}, device_id_type=MESH).start()
        return 0

    lax.fori_loop(1, 32, tell, 0)
    others = parts.at[pl.ds(0, 31)]
    pltpu.make_async_copy(others, others, norm_recv).wait()
    norm[...] = jnp.sum(parts[...], axis=0)
    pltpu.make_async_copy(others, others, norm_send).wait()

    def drain(t, _):
        for a in range(2):
            pltpu.make_async_copy(pair.at[t, a], pair.at[t, a], pair_send.at[t, a]).wait()
            for s in range(4):
                sent = slots.at[t, a, pl.ds(START[s], COUNT[s])]
                pltpu.make_async_copy(sent, sent, send.at[t, a, s]).wait()
        return 0

    lax.fori_loop(0, ROUNDS, drain, 0)


def unit_loads(sources, buffers, sems, i, layer):
    u = 2 * i + layer
    return [pltpu.make_async_copy(one[i].at[layer], here.at[u], sems.at[u, n]) for n, (one, here) in enumerate(zip(sources, buffers, strict=True))]


def factor_of(norm, count):
    squares = jnp.full((ROWS, 128), jnp.sum(norm[...]), jnp.float32)
    return jnp.minimum(1.0, 0.5 * lax.rsqrt(squares / count + 1e-30))


UNITS = ((0, 0), (1, 0), (2, 0), (2, 1), (0, 1), (1, 1))


def gather_kernel(size, norm, g, w, m, v, gate, up, down, g_now, w_now, m_now, v_now, got, own_sem, pair_send, pair_recv, send, recv):
    me, k, c = place()
    sources, buffers = (g, [one.at[:, me] for one in w], m, v), (g_now, w_now, m_now, v_now)
    for i, layer in UNITS:
        for one in unit_loads(sources, buffers, got, i, layer):
            one.start()
    factor = factor_of(norm, size)

    def block(w_down, t, a, chip, core, count=None):
        chip = chip if count is None else pl.ds(chip, count)
        layer, part, down_part = source(t)
        ref, layer, part = (down, a, down_part) if w_down else ((gate, up)[a], layer, part)
        return ref.at[layer, chip, core, pl.ds(part * PART, PART)]

    def chips(a, s, at):
        b = bits(a)[::-1]
        base = at
        for i in range(s):
            base = base - bit(at, b[i]) * b[i]

        def chip_of(j):
            chip = base
            for i in range(s):
                chip = chip + bit(j, 2**i) * b[i]
            return chip

        return chip_of

    def own_part(w_down, t, a):
        layer, part, down_part = source(t)
        i, layer, part = (2, a, down_part) if w_down else (a, layer, part)
        return i, layer, part, w_now.at[2 * i + layer, pl.ds(part * PART, PART)]

    def own_block(w_down, t, a):
        return pltpu.make_async_copy(own_part(w_down, t, a)[3], block(w_down, t, a, k, c), own_sem.at[t, a])

    def renew(w_down, t, a):
        i, layer, part, mine = own_part(w_down, t, a)

        @pl.when(part == 0)
        def _():
            for one in unit_loads(sources, buffers, got, i, layer):
                one.wait()

        u, at = 2 * i + layer, pl.ds(part * PART, PART)
        gradient = g_now[u, at].astype(jnp.float32) * factor
        mine[...] = adamw(mine[...].astype(jnp.float32), m_now[u, at], v_now[u, at], gradient)[0]

    def stage(w_down, t, a, s):
        if s == 0:
            mine = own_part(w_down, t, a)[3]
            own_block(w_down, t, a).start()
            there = block(w_down, t, a, k, c)
            copy_to(mine, there, send.at[t, a, 0], recv.at[t, a, 0], flip(k, bits(a)[3]), c).start()
            copy_to(mine, there, pair_send.at[t, a], pair_recv.at[t, a], k, 1 - c).start()
            return
        if s == 1:
            own_block(w_down, t, a).wait()
        count = 2 ** (s - 1)
        size = block(w_down, t, a, 0, 0, count)
        pltpu.make_async_copy(size, size, recv.at[t, a, s - 1]).wait()
        fresh = chips(a, s - 1, flip(k, bits(a)[4 - s]))
        if s < 4:
            of, other = chips(a, s, k), flip(k, bits(a)[3 - s])

            def go(j, _):
                one = block(w_down, t, a, of(j), c)
                copy_to(one, one, send.at[t, a, s], recv.at[t, a, s], other, c).start()
                return 0

            lax.fori_loop(0, 2**s, go, 0)

        def share(j, _):
            one = block(w_down, t, a, fresh(j), c)
            copy_to(one, one, pair_send.at[t, a], pair_recv.at[t, a], k, 1 - c).start()
            return 0

        lax.fori_loop(0, count, share, 0)

    def step(now, _):
        for s in range(5):
            t = now - GATHER_LAG[s]

            @pl.when((t >= 0) & (t < ROUNDS))
            def _():
                def go(w_down):
                    if s == 0:
                        for a in range(2):
                            renew(w_down, t, a)
                    for a in range(2):
                        stage(w_down, t, a, s)

                by_kind(t, go)

        return 0

    lax.fori_loop(0, ROUNDS + GATHER_LAG[4], step, 0)

    def drain(t, _):
        for a in range(2):
            for sems, s in ((pair_recv.at[t, a], 4), (pair_send.at[t, a], 4), *((send.at[t, a, s], s) for s in range(4))):
                size = gate.at[0, pl.ds(0, 2**s), 0, pl.ds(0, PART)]
                pltpu.make_async_copy(size, size, sems).wait()
        return 0

    lax.fori_loop(0, ROUNDS, drain, 0)


def store_kernel(size, norm, g, m, v, whole, w_out, m_out, v_out, g_now, m_now, v_now, got, put, put_whole):
    sources, buffers = (g, m, v), (g_now, m_now, v_now)
    for i, layer in UNITS:
        for one in unit_loads(sources, buffers, got, i, layer):
            one.start()
    stores = [pltpu.make_async_copy(whole[i].at[layer], w_out[i].at[layer], put_whole.at[2 * i + layer]) for i, layer in UNITS]
    for one in stores:
        one.start()
    factor = factor_of(norm, size)
    for i, layer in UNITS:
        for one in unit_loads(sources, buffers, got, i, layer):
            one.wait()
        u = 2 * i + layer

        def go(j, _):
            at = pl.ds(j * PART, PART)
            gradient = g_now[u, at].astype(jnp.float32) * factor
            _, m_now[u, at], v_now[u, at] = adamw(jnp.zeros((), jnp.float32), m_now[u, at], v_now[u, at], gradient)
            return 0

        lax.fori_loop(0, PARTS, go, 0)
        for n, (here, there) in enumerate(((m_now, m_out), (v_now, v_out))):
            stores.append(pltpu.make_async_copy(here.at[u], there[i].at[layer], put.at[u, n]))
            stores[-1].start()
    for one in stores:
        one.wait()


def adamw(w, m, v, g):
    m = 0.9 * m + 0.1 * g
    v = 0.95 * v + 0.05 * g * g
    step = m * lax.rsqrt(v + 1e-8) + 0.1 * w
    return (w - 0.02 * step).astype(jnp.bfloat16), m, v


def stay(one):
    return pltpu.with_memory_space_constraint(one, pltpu.HBM)


def solution(mesh):
    hbm, vmem = (pl.BlockSpec(memory_space=one) for one in (pl.ANY, pltpu.VMEM))
    dma = pltpu.SemaphoreType.DMA
    params = pltpu.CompilerParams(has_side_effects=True, vmem_limit_bytes=67043328)

    def step(*arrays):
        terms, weights, m, v = (arrays[i : i + 3] for i in (0, 3, 6, 9))
        tile = (ROWS, 128)
        terms = [view(t[0]).reshape(2, CHIPS, 2, TILES, *tile) for t in terms]
        *g, norm = pl.pallas_call(
            sum_kernel,
            out_shape=[*[jax.ShapeDtypeStruct((2, TILES, *tile), jnp.bfloat16)] * 3, jax.ShapeDtypeStruct(tile, jnp.float32)],
            in_specs=[hbm] * 3,
            out_specs=[vmem] * 4,
            scratch_shapes=[
                pltpu.VMEM((ROUNDS, 2, CHIPS, PART, *tile), jnp.bfloat16),
                pltpu.VMEM((ROUNDS, 2, CHIPS, PART, *tile), jnp.bfloat16),
                pltpu.VMEM((ROUNDS, 2, 15, PART, *tile), jnp.bfloat16),
                pltpu.VMEM(tile, jnp.float32),
                pltpu.VMEM((32, *tile), jnp.float32),
                dma((ROUNDS, 2)),
                dma((ROUNDS, 2)),
                dma((ROUNDS, 2)),
                dma((ROUNDS, 2, 4)),
                dma((ROUNDS, 2, 4)),
                dma,
                dma,
            ],
            compiler_params=params,
        )(*terms)
        count = 32 * sum(one.size for one in m)

        def gather(norm, *refs):
            threes = [refs[i : i + 3] for i in (0, 3, 6, 9)]
            gather_kernel(count, norm, *threes, *refs[12:])

        def store(norm, *refs):
            threes = [refs[i : i + 3] for i in range(0, 21, 3)]
            store_kernel(count, norm, *threes, *refs[21:])

        mine = (2, TILES, *tile)
        blocks = [jax.ShapeDtypeStruct((2, CHIPS, 2, TILES, *tile), jnp.bfloat16)] * 3
        m, v = ([view(one)[:, 0] for one in them] for them in (m, v))
        narrow, wide = pltpu.VMEM((6, TILES, *tile), jnp.bfloat16), pltpu.VMEM((6, TILES, *tile), jnp.float32)
        whole = pl.pallas_call(
            gather,
            out_shape=blocks,
            in_specs=[vmem] + [hbm] * 12,
            out_specs=[hbm] * 3,
            scratch_shapes=[
                narrow,
                narrow,
                wide,
                wide,
                dma((6, 4)),
                dma((ROUNDS, 2)),
                dma((ROUNDS, 2)),
                dma((ROUNDS, 2)),
                dma((ROUNDS, 2, 4)),
                dma((ROUNDS, 2, 4)),
            ],
            compiler_params=pltpu.CompilerParams(has_side_effects=True, vmem_limit_bytes=LIMIT << 20),
        )(norm, *map(stay, (*g, *(view(one) for one in weights), *m, *v)))
        *whole, m0, m1, m2, v0, v1, v2 = pl.pallas_call(
            store,
            out_shape=blocks + [jax.ShapeDtypeStruct(mine, jnp.float32)] * 6,
            in_specs=[vmem] + [hbm] * 12,
            out_specs=[hbm] * 9,
            scratch_shapes=[narrow, wide, wide, dma((6, 3)), dma((6, 2)), dma((6,))],
            compiler_params=pltpu.CompilerParams(vmem_limit_bytes=LIMIT << 20),
        )(norm, *map(stay, (*g, *m, *v)), *whole)
        whole = [unview(one, w.shape) for one, w in zip(whole, weights, strict=True)]
        moments = [unview(one, like.shape) for one, like in zip((m0, m1, m2, v0, v1, v2), arrays[6:], strict=True)]
        return (*whole, *moments)

    all_of, cut = P(None, None, None), P(None, "dp", None)
    return jax.shard_map(
        step,
        mesh=mesh,
        in_specs=(P(("rep", "dp"), None, None, None),) * 3 + (all_of,) * 3 + (cut,) * 6,
        out_specs=(P("rep", None, None),) * 3 + (P("rep", "dp", None),) * 6,
        check_vma=False,
    )
```

```python
import functools

import jax
import jax.numpy as jnp
from jax import lax
from jax.experimental import pallas as pl
from jax.experimental.pallas import tpu as pltpu
from jax.sharding import PartitionSpec as P

MESH = pl.DeviceIdType.MESH
CHIPS = 16
ROWS, TILES, PART = 8, 104, 13
PARTS = TILES // PART
ROUNDS = 3 * PARTS
START, COUNT = (0, 8, 12, 14), (8, 4, 2, 1)
AHEAD = 3
LIMIT = 12
SUM_LAG = (0, 2, 3, 4, 5)
GATHER_LAG = (0, 1, 2, 3, 4)


def view(t):
    layers, rows, columns = t.shape
    return t.reshape(layers, rows // 8, 8, columns // 128, 128).transpose(0, 1, 3, 2, 4).reshape(layers, -1, TILES, ROWS, 128)


def unview(t, shape):
    layers, rows, columns = shape
    return t.reshape(layers, rows // 8, columns // 128, 8, 128).transpose(0, 1, 3, 2, 4).reshape(shape)


def place():
    me = lax.axis_index("dp")
    return me, me // 2, me % 2


def is_down(t):
    return (t % 3) // 2


def source(t):
    i = 2 * (t // 3) + t % 3
    return i // PARTS, i % PARTS, t // 3


def bits(a):
    return ((8, 1, 4, 2), (4, 1, 8, 2))[a]


def by_kind(t, do):
    for down in (False, True):
        pl.when(is_down(t) == int(down))(functools.partial(do, down))


def bit(k, b):
    return (k // b) % 2


def flip(k, b):
    return k + (1 - 2 * bit(k, b)) * b


def copy_to(src, dst, send, recv, chip, core):
    return pltpu.make_async_remote_copy(src_ref=src, dst_ref=dst, send_sem=send, recv_sem=recv, device_id={"dp": 2 * chip + core}, device_id_type=MESH)


def sum_kernel(gate, up, down, gate_out, up_out, down_out, norm, own, pair, slots, squares, parts, own_sem, pair_send, pair_recv, send, recv, norm_send, norm_recv):
    me, k, c = place()

    def load(t):
        def go(w_down):
            layer, part, down_part = source(t)
            for a in range(2):
                ref, layer_a, part_a = (down, a, down_part) if w_down else ((gate, up)[a], layer, part)
                at = pl.ds(part_a * PART, PART)
                copy_to(ref.at[layer_a, :, 1 - c, at], pair.at[t, a], pair_send.at[t, a], pair_recv.at[t, a], k, 1 - c).start()
                pltpu.make_async_copy(ref.at[layer_a, :, c, at], own.at[t, a], own_sem.at[t, a]).start()

        by_kind(t, go)

    lax.fori_loop(0, AHEAD, lambda t, _: load(t), None)
    squares[...] = jnp.zeros_like(squares)

    def await_slots(t, a, s):
        got = slots.at[t, a, pl.ds(START[s], COUNT[s])]
        pltpu.make_async_copy(got, got, recv.at[t, a, s]).wait()

    def total(t, a, s, chip):
        b = bits(a)
        so_far = own[t, a, chip].astype(jnp.float32) + pair[t, a, chip].astype(jnp.float32)
        for i in range(s):
            index = START[i]
            for j in range(i + 1, 4):
                index = index + bit(chip, b[j]) * 2 ** (3 - j)
            so_far = so_far + slots[t, a, index].astype(jnp.float32)
        return so_far

    def stage(t, a, s):
        b = bits(a)
        other = flip(k, b[s])
        if s == 0:
            pltpu.make_async_copy(own.at[t, a], own.at[t, a], own_sem.at[t, a]).wait()
            pltpu.make_async_copy(pair.at[t, a], pair.at[t, a], pair_recv.at[t, a]).wait()
        else:
            await_slots(t, a, s - 1)
        base = other
        for i in range(s + 1, 4):
            base = base - bit(other, b[i]) * b[i]

        def chip_of(j):
            chip = base
            for i in range(s + 1, 4):
                chip = chip + bit(j, 2 ** (3 - i)) * b[i]
            return chip

        def add(j, _):
            chip = chip_of(j)
            own[t, a, chip] = total(t, a, s, chip).astype(jnp.bfloat16)
            return 0

        def go(j, _):
            copy_to(own.at[t, a, chip_of(j)], slots.at[t, a, START[s] + j], send.at[t, a, s], recv.at[t, a, s], other, c).start()
            return 0

        def add_and_go(j, _):
            add(j, 0)
            go(j - 1, 0)
            return 0

        add(0, 0)
        lax.fori_loop(1, COUNT[s], add_and_go, 0)
        go(COUNT[s] - 1, 0)

    def finish(t, a):
        await_slots(t, a, 3)
        g = total(t, a, 4, k).astype(jnp.bfloat16)

        def put(w_down):
            layer, part, down_part = source(t)
            out, layer, part = (down_out, a, down_part) if w_down else ((gate_out, up_out)[a], layer, part)
            out[layer, pl.ds(part * PART, PART)] = g

        by_kind(t, put)
        g = g.astype(jnp.float32)
        squares[...] += jnp.sum(g * g, axis=0)

    def step(now, _):
        pl.when(now + AHEAD < ROUNDS)(lambda: load(now + AHEAD))
        for s in range(5):
            t = now - SUM_LAG[s]

            @pl.when((t >= 0) & (t < ROUNDS))
            def _():
                for a in range(2):
                    if s < 4:
                        stage(t, a, s)
                    else:
                        finish(t, a)

        return 0

    lax.fori_loop(0, ROUNDS + SUM_LAG[4], step, 0)

    mine = parts.at[me]
    mine[...] = squares[...]

    def tell(i, _):
        to = (me + i) % 32
        pltpu.make_async_remote_copy(src_ref=squares, dst_ref=mine, send_sem=norm_send, recv_sem=norm_recv, device_id={"dp": to}, device_id_type=MESH).start()
        return 0

    lax.fori_loop(1, 32, tell, 0)
    others = parts.at[pl.ds(0, 31)]
    pltpu.make_async_copy(others, others, norm_recv).wait()
    norm[...] = jnp.sum(parts[...], axis=0)
    pltpu.make_async_copy(others, others, norm_send).wait()

    def drain(t, _):
        for a in range(2):
            pltpu.make_async_copy(pair.at[t, a], pair.at[t, a], pair_send.at[t, a]).wait()
            for s in range(4):
                sent = slots.at[t, a, pl.ds(START[s], COUNT[s])]
                pltpu.make_async_copy(sent, sent, send.at[t, a, s]).wait()
        return 0

    lax.fori_loop(0, ROUNDS, drain, 0)


def unit_loads(sources, buffers, sems, i, layer):
    u = 2 * i + layer
    return [pltpu.make_async_copy(one[i].at[layer], here.at[u], sems.at[u, n]) for n, (one, here) in enumerate(zip(sources, buffers, strict=True))]


def factor_of(norm, count):
    squares = jnp.full((ROWS, 128), jnp.sum(norm[...]), jnp.float32)
    return jnp.minimum(1.0, 0.5 * lax.rsqrt(squares / count + 1e-30))


UNITS = ((0, 0), (1, 0), (2, 0), (2, 1), (0, 1), (1, 1))


def gather_kernel(size, norm, g, w, m, v, gate, up, down, g_now, w_now, m_now, v_now, got, own_sem, pair_send, pair_recv, send, recv):
    me, k, c = place()
    sources, buffers = (g, [one.at[:, me] for one in w], m, v), (g_now, w_now, m_now, v_now)
    for i, layer in UNITS:
        for one in unit_loads(sources, buffers, got, i, layer):
            one.start()
    factor = factor_of(norm, size)

    def block(w_down, t, a, chip, core, count=None):
        chip = chip if count is None else pl.ds(chip, count)
        layer, part, down_part = source(t)
        ref, layer, part = (down, a, down_part) if w_down else ((gate, up)[a], layer, part)
        return ref.at[layer, chip, core, pl.ds(part * PART, PART)]

    def chips(a, s, at):
        b = bits(a)[::-1]
        base = at
        for i in range(s):
            base = base - bit(at, b[i]) * b[i]

        def chip_of(j):
            chip = base
            for i in range(s):
                chip = chip + bit(j, 2**i) * b[i]
            return chip

        return chip_of

    def own_part(w_down, t, a):
        layer, part, down_part = source(t)
        i, layer, part = (2, a, down_part) if w_down else (a, layer, part)
        return i, layer, part, w_now.at[2 * i + layer, pl.ds(part * PART, PART)]

    def own_block(w_down, t, a):
        return pltpu.make_async_copy(own_part(w_down, t, a)[3], block(w_down, t, a, k, c), own_sem.at[t, a])

    def renew(w_down, t, a):
        i, layer, part, mine = own_part(w_down, t, a)

        @pl.when(part == 0)
        def _():
            for one in unit_loads(sources, buffers, got, i, layer):
                one.wait()

        u, at = 2 * i + layer, pl.ds(part * PART, PART)
        gradient = g_now[u, at].astype(jnp.float32) * factor
        mine[...] = adamw(mine[...].astype(jnp.float32), m_now[u, at], v_now[u, at], gradient)[0]

    def stage(w_down, t, a, s):
        if s == 0:
            mine = own_part(w_down, t, a)[3]
            own_block(w_down, t, a).start()
            there = block(w_down, t, a, k, c)
            copy_to(mine, there, send.at[t, a, 0], recv.at[t, a, 0], flip(k, bits(a)[3]), c).start()
            copy_to(mine, there, pair_send.at[t, a], pair_recv.at[t, a], k, 1 - c).start()
            return
        if s == 1:
            own_block(w_down, t, a).wait()
        count = 2 ** (s - 1)
        size = block(w_down, t, a, 0, 0, count)
        pltpu.make_async_copy(size, size, recv.at[t, a, s - 1]).wait()
        fresh = chips(a, s - 1, flip(k, bits(a)[4 - s]))
        if s < 4:
            of, other = chips(a, s, k), flip(k, bits(a)[3 - s])

            def go(j, _):
                one = block(w_down, t, a, of(j), c)
                copy_to(one, one, send.at[t, a, s], recv.at[t, a, s], other, c).start()
                return 0

            lax.fori_loop(0, 2**s, go, 0)

        def share(j, _):
            one = block(w_down, t, a, fresh(j), c)
            copy_to(one, one, pair_send.at[t, a], pair_recv.at[t, a], k, 1 - c).start()
            return 0

        lax.fori_loop(0, count, share, 0)

    def step(now, _):
        for s in range(5):
            t = now - GATHER_LAG[s]

            @pl.when((t >= 0) & (t < ROUNDS))
            def _():
                def go(w_down):
                    if s == 0:
                        for a in range(2):
                            renew(w_down, t, a)
                    for a in range(2):
                        stage(w_down, t, a, s)

                by_kind(t, go)

        return 0

    lax.fori_loop(0, ROUNDS + GATHER_LAG[4], step, 0)

    def drain(t, _):
        for a in range(2):
            for sems, s in ((pair_recv.at[t, a], 4), (pair_send.at[t, a], 4), *((send.at[t, a, s], s) for s in range(4))):
                size = gate.at[0, pl.ds(0, 2**s), 0, pl.ds(0, PART)]
                pltpu.make_async_copy(size, size, sems).wait()
        return 0

    lax.fori_loop(0, ROUNDS, drain, 0)


def store_kernel(size, norm, g, m, v, whole, w_out, m_out, v_out, g_now, m_now, v_now, got, put, put_whole):
    sources, buffers = (g, m, v), (g_now, m_now, v_now)
    for i, layer in UNITS:
        for one in unit_loads(sources, buffers, got, i, layer):
            one.start()
    stores = [pltpu.make_async_copy(whole[i].at[layer], w_out[i].at[layer], put_whole.at[2 * i + layer]) for i, layer in UNITS]
    for one in stores:
        one.start()
    factor = factor_of(norm, size)
    for i, layer in UNITS:
        for one in unit_loads(sources, buffers, got, i, layer):
            one.wait()
        u = 2 * i + layer

        def go(j, _):
            at = pl.ds(j * PART, PART)
            gradient = g_now[u, at].astype(jnp.float32) * factor
            _, m_now[u, at], v_now[u, at] = adamw(jnp.zeros((), jnp.float32), m_now[u, at], v_now[u, at], gradient)
            return 0

        lax.fori_loop(0, PARTS, go, 0)
        for n, (here, there) in enumerate(((m_now, m_out), (v_now, v_out))):
            stores.append(pltpu.make_async_copy(here.at[u], there[i].at[layer], put.at[u, n]))
            stores[-1].start()
    for one in stores:
        one.wait()


def adamw(w, m, v, g):
    m = 0.9 * m + 0.1 * g
    v = 0.95 * v + 0.05 * g * g
    step = m * lax.rsqrt(v + 1e-8) + 0.1 * w
    return (w - 0.02 * step).astype(jnp.bfloat16), m, v


def stay(one):
    return pltpu.with_memory_space_constraint(one, pltpu.HBM)


def solution(mesh):
    hbm, vmem = (pl.BlockSpec(memory_space=one) for one in (pl.ANY, pltpu.VMEM))
    dma = pltpu.SemaphoreType.DMA
    params = pltpu.CompilerParams(has_side_effects=True, vmem_limit_bytes=67043328)

    def step(*arrays):
        terms, weights, m, v = (arrays[i : i + 3] for i in (0, 3, 6, 9))
        tile = (ROWS, 128)
        terms = [view(t[0]).reshape(2, CHIPS, 2, TILES, *tile) for t in terms]
        *g, norm = pl.pallas_call(
            sum_kernel,
            out_shape=[*[jax.ShapeDtypeStruct((2, TILES, *tile), jnp.bfloat16)] * 3, jax.ShapeDtypeStruct(tile, jnp.float32)],
            in_specs=[hbm] * 3,
            out_specs=[vmem] * 4,
            scratch_shapes=[
                pltpu.VMEM((ROUNDS, 2, CHIPS, PART, *tile), jnp.bfloat16),
                pltpu.VMEM((ROUNDS, 2, CHIPS, PART, *tile), jnp.bfloat16),
                pltpu.VMEM((ROUNDS, 2, 15, PART, *tile), jnp.bfloat16),
                pltpu.VMEM(tile, jnp.float32),
                pltpu.VMEM((32, *tile), jnp.float32),
                dma((ROUNDS, 2)),
                dma((ROUNDS, 2)),
                dma((ROUNDS, 2)),
                dma((ROUNDS, 2, 4)),
                dma((ROUNDS, 2, 4)),
                dma,
                dma,
            ],
            compiler_params=params,
        )(*terms)
        count = 32 * sum(one.size for one in m)

        def gather(norm, *refs):
            threes = [refs[i : i + 3] for i in (0, 3, 6, 9)]
            gather_kernel(count, norm, *threes, *refs[12:])

        def store(norm, *refs):
            threes = [refs[i : i + 3] for i in range(0, 21, 3)]
            store_kernel(count, norm, *threes, *refs[21:])

        mine = (2, TILES, *tile)
        blocks = [jax.ShapeDtypeStruct((2, CHIPS, 2, TILES, *tile), jnp.bfloat16)] * 3
        m, v = ([view(one)[:, 0] for one in them] for them in (m, v))
        narrow, wide = pltpu.VMEM((6, TILES, *tile), jnp.bfloat16), pltpu.VMEM((6, TILES, *tile), jnp.float32)
        whole = pl.pallas_call(
            gather,
            out_shape=blocks,
            in_specs=[vmem] + [hbm] * 12,
            out_specs=[hbm] * 3,
            scratch_shapes=[
                narrow,
                narrow,
                wide,
                wide,
                dma((6, 4)),
                dma((ROUNDS, 2)),
                dma((ROUNDS, 2)),
                dma((ROUNDS, 2)),
                dma((ROUNDS, 2, 4)),
                dma((ROUNDS, 2, 4)),
            ],
            compiler_params=pltpu.CompilerParams(has_side_effects=True, vmem_limit_bytes=LIMIT << 20),
        )(norm, *map(stay, (*g, *(view(one) for one in weights), *m, *v)))
        *whole, m0, m1, m2, v0, v1, v2 = pl.pallas_call(
            store,
            out_shape=blocks + [jax.ShapeDtypeStruct(mine, jnp.float32)] * 6,
            in_specs=[vmem] + [hbm] * 12,
            out_specs=[hbm] * 9,
            scratch_shapes=[narrow, wide, wide, dma((6, 3)), dma((6, 2)), dma((6,))],
            compiler_params=pltpu.CompilerParams(vmem_limit_bytes=LIMIT << 20),
        )(norm, *map(stay, (*g, *m, *v)), *whole)
        whole = [unview(one, w.shape) for one, w in zip(whole, weights, strict=True)]
        moments = [unview(one, like.shape) for one, like in zip((m0, m1, m2, v0, v1, v2), arrays[6:], strict=True)]
        return (*whole, *moments)

    all_of, cut = P(None, None, None), P(None, "dp", None)
    return jax.shard_map(
        step,
        mesh=mesh,
        in_specs=(P(("rep", "dp"), None, None, None),) * 3 + (all_of,) * 3 + (cut,) * 6,
        out_specs=(P("rep", None, None),) * 3 + (P("rep", "dp", None),) * 6,
        check_vma=False,
    )
```
